32 devices in a mesh: sweep: 2 (over y), row: 4 (over z), col: 2 (over x), dp: 2 (over core).
Axes of the slice: x: 2, y: 2, z: 4, core: 2. Of those that a mesh axis runs over, the one named last changes fastest.
Arguments:
- token_ids: int32 [4096], P(('sweep', 'dp')), parts along dimension 0, may hold values from 0 to 15999
- sweep_index: int32 [4], P('sweep'), parts along dimension 0, may hold values from 0 to 7
- table: bfloat16 [16000, 4096], P('row', 'col'), may hold values from -6 to 6
- cotangent: bfloat16 [4096, 4096], P(('sweep', 'dp', 'row'), 'col'), parts along dimension 0, may hold values from -0.13183594 to 0.13183594
- gate_weight: bfloat16 [4096, 11008], P('col', 'row'), may hold values from -0.09375 to 0.09375
- up_weight: bfloat16 [4096, 11008], P('col', 'row'), may hold values from -0.09375 to 0.09375
- down_weight: bfloat16 [11008, 4096], P('row', 'col'), may hold values from -0.0546875 to 0.0546875
Outputs:
- grad_gate: float32 [8192, 11008], P(('sweep', 'col'), ('row', 'dp')), parts along dimension 0
- grad_up: float32 [8192, 11008], P(('sweep', 'col'), ('row', 'dp')), parts along dimension 0
- grad_down: float32 [22016, 4096], P(('sweep', 'row'), ('col', 'dp')), parts along dimension 0
The draws below stay inside these ranges and needn't reach their ends.
There are 2 independent parts, one for each index of `sweep`. The reference program is written for one: setup_inputs(seed, part) draws one part's arguments, and reference() takes and returns one part's arrays. A program takes and returns all parts, laid end to end along the dimension named above; an argument that names none is the same for every part. Nothing has to cross between parts.
All inputs are finite; a program needn't handle non-finite values.
Results may differ from the reference program's by a relative error of at most 0.0062.
Values may be sent and summed in bfloat16 or wider, within the bound.
A program may use at most 256 MiB of HBM per device.

```python
import math
import jax
import jax.numpy as jnp
import numpy as np

D = 4096
FF = 11008
VOCAB = 16000
TOKENS = 2048


def touch_ends(entries, own_key, smallest, top_value):
    dims = entries.shape
    place = [jax.random.randint(jax.random.fold_in(own_key, axis), (), 0, dims[axis]) for axis in range(len(dims))]
    entries = entries.at[tuple(place)].set(smallest)
    longest = dims.index(max(dims))
    place[longest] = (place[longest] + 1) % dims[longest]
    return entries.at[tuple(place)].set(top_value)


def levels(stream_key, extent, shards, smallest, high):
    loudness, own = 1.0, jax.random.fold_in(stream_key, 6)
    for position, blocks in shards:
        draws = jnp.exp(jax.random.uniform(jax.random.fold_in(own, position), (blocks,), jnp.float32, smallest / len(shards), high / len(shards)))
        loudness = loudness * jnp.repeat(draws, extent[position] // blocks).reshape([-1 if axis == position else 1 for axis in range(len(extent))])
    return loudness


def rank_bounds(amount, lean):
    weights = [(1 << 20) // math.isqrt(grade ** lean) + 1 for grade in range(1, amount + 1)]
    width = 1 + sum(weights) // (1 << 30)
    return np.cumsum(np.array([max(1, weight // width) for weight in weights]))


def ranked_ids(own_key, dims, amount, slope):
    listing = rank_bounds(amount, slope)
    lot = jax.random.randint(jax.random.fold_in(own_key, 1), dims, 0, int(listing[amount - 1]))
    grade = jnp.searchsorted(jnp.asarray(listing, jnp.int32), lot, side="right")
    return jax.random.permutation(jax.random.fold_in(own_key, 2), amount)[grade].astype(jnp.int32)


def noise(rng, shape, width, reach, split=(), kind=jnp.bfloat16):
    entries = width * jax.random.normal(rng, shape, jnp.float32)
    if split:
        entries = entries * levels(rng, shape, split, -0.22, 0.18)
    return jnp.clip(entries, -reach, reach).astype(kind)


def setup_inputs(seed: int = 0, part: int = 0) -> dict:
    arg_keys = jax.random.split(jax.random.key(seed), 8)
    part_keys = jax.random.split(jax.random.fold_in(arg_keys[7], part), 8)
    token_ids = touch_ends(ranked_ids(part_keys[0], (TOKENS,), VOCAB, 2), jax.random.fold_in(part_keys[0], 3), 0, VOCAB - 1).astype(jnp.int32)
    sweep_index = jax.random.randint(part_keys[1], (2,), 0, 8).astype(jnp.int32)
    table = noise(arg_keys[2], (VOCAB, D), 1.0, 6.0, ((0, 4), (1, 2)))
    cotangent = noise(part_keys[3], (TOKENS, D), (TOKENS ** -0.5), 0.13183594, ((0, 8), (1, 2)))
    gate_weight = noise(arg_keys[4], (D, FF), D ** -0.5, 0.09375, ((0, 2), (1, 4)))
    up_weight = noise(arg_keys[5], (D, FF), D ** -0.5, 0.09375, ((0, 2), (1, 4)))
    down_weight = noise(arg_keys[6], (FF, D), FF ** -0.5, 0.0546875, ((0, 4), (1, 2)))
    return {"token_ids": token_ids, "sweep_index": sweep_index, "table": table, "cotangent": cotangent, "gate_weight": gate_weight, "up_weight": up_weight, "down_weight": down_weight}


def reference(token_ids, sweep_index, table, cotangent, gate_weight, up_weight, down_weight):
    k_input = sweep_index[0].astype(jnp.float32)
    k_output = sweep_index[1].astype(jnp.float32)
    in_mult = jnp.exp2(k_input / 2.0 - 1.5)
    out_mult = jnp.exp2(1.0 - k_output / 2.0)
    embedded = jnp.take(table, token_ids, axis=0)
    scaled = (in_mult * embedded.astype(jnp.float32)).astype(jnp.bfloat16)
    gate = jnp.dot(scaled, gate_weight, preferred_element_type=jnp.float32)
    up = jnp.dot(scaled, up_weight, preferred_element_type=jnp.float32)
    back = out_mult * jnp.dot(cotangent, down_weight.T, preferred_element_type=jnp.float32)
    sig = jax.nn.sigmoid(gate)
    silu = gate * sig
    hidden = (silu * up).astype(jnp.bfloat16)
    d_gate = (back * up * sig * (1.0 + gate * (1.0 - sig))).astype(jnp.bfloat16)
    d_up = (back * silu).astype(jnp.bfloat16)
    grad_down = out_mult * jnp.dot(hidden.T, cotangent, preferred_element_type=jnp.float32)
    grad_gate = jnp.dot(scaled.T, d_gate, preferred_element_type=jnp.float32)
    grad_up = jnp.dot(scaled.T, d_up, preferred_element_type=jnp.float32)
    return grad_gate, grad_up, grad_down
```

```python
import jax
import jax.numpy as jnp
from jax import lax
from jax.sharding import PartitionSpec as P


def dot(left, right, dims):
    return lax.dot_general(left, right, (dims, ((), ())), preferred_element_type=jnp.float32)


ROWS = ((0,), (0,))
COLS = ((1,), (1,))
PLAIN = ((1,), (0,))


def shift(value, axis, size, step):
    return lax.ppermute(value, axis, [((i + step) % size, i) for i in range(size)])


def line_sum(own, axis, size):
    up, down = own, own
    above = below = None
    for k in range(size - 1):
        got = lax.ppermute(up, axis, [(k, k + 1)])
        below = got if below is None else below + got
        up = own + below
        got = lax.ppermute(down, axis, [(size - 1 - k, size - 2 - k)])
        above = got if above is None else above + got
        down = own + above
    return own if below is None else own + below + above


def line_gather(own, axis, size):
    me = lax.axis_index(axis)
    up, down = [own], [own]
    for k in range(1, size):
        up.append(lax.ppermute(up[-1], axis, [(i, i + 1) for i in range(k - 1, size - 1)]))
        down.append(lax.ppermute(down[-1], axis, [(i + 1, i) for i in range(size - k)]))
    rows = own.shape[0]
    out = jnp.zeros((size * rows, own.shape[1]), own.dtype)
    for k in range(size):
        block = own if k == 0 else jnp.where(me + k < size, down[k], up[size - k])
        out = lax.dynamic_update_slice(out, block, (lax.rem(me + k, size) * rows, 0))
    return out


def build(mesh):
    n_sweep, n_row, n_col, n_dp = (mesh.shape[a] for a in ("sweep", "row", "col", "dp"))

    def local(token_ids, sweep_index, table, cotangent, gate_weight, up_weight, down_weight):
        in_mult = jnp.exp2(sweep_index[0].astype(jnp.float32) / 2.0 - 1.5)
        out_mult = jnp.exp2(1.0 - sweep_index[1].astype(jnp.float32) / 2.0)
        s, r, d = (lax.axis_index(a) for a in ("sweep", "row", "dp"))
        feats = table.shape[1]
        width = gate_weight.shape[1] // n_dp
        part = feats // n_sweep
        others = range(1, n_col)

        crossed = [cotangent] + [shift(cotangent, "col", n_col, k) for k in others]

        def fetch(piece):
            got = []
            for k in others:
                first = shift(piece, "col", n_col, k)
                got.append([first] + [shift(first, "sweep", n_sweep, j) for j in range(1, n_sweep)])
            return got

        gate_piece = lax.dynamic_slice(gate_weight, (s * part, d * width), (part, width))
        up_piece = lax.dynamic_slice(up_weight, (s * part, d * width), (part, width))
        down_piece = lax.dynamic_slice(down_weight, (d * width, s * part), (width, part))
        gate_own = lax.dynamic_slice(gate_weight, (0, d * width), (feats, width))
        up_own = lax.dynamic_slice(up_weight, (0, d * width), (feats, width))
        down_own = lax.dynamic_slice(down_weight, (d * width, 0), (width, feats))
        gate_far = fetch(gate_piece)
        up_far = fetch(up_piece)

        table_rows = table.shape[0]
        blocks = 4
        count = token_ids.shape[0] // blocks
        scaled_blocks = []
        for b in range(blocks):
            offset = token_ids[b * count : (b + 1) * count] - r * table_rows
            inside = jnp.logical_and(offset >= 0, offset < table_rows)
            picked = jnp.take(table, jnp.clip(offset, 0, table_rows - 1), axis=0)
            looked = jnp.where(inside[:, None], picked, jnp.zeros((), jnp.bfloat16))
            embedded = line_sum(looked, "row", n_row).astype(jnp.float32)
            scaled_blocks.append((in_mult * embedded).astype(jnp.bfloat16))
        x_own = lax.all_gather(jnp.concatenate(scaled_blocks, 0), "dp", axis=0, tiled=True)
        x_far = [
            lax.all_gather(
                jnp.concatenate([shift(x, "col", n_col, k) for x in scaled_blocks], 0),
                "dp", axis=0, tiled=True,
            )
            for k in others
        ]

        down_piece, _ = lax.optimization_barrier((down_piece, scaled_blocks[-1]))
        cuts = 4 if width % 4 == 0 else 1
        step = width // cuts
        fetched = [fetch(down_piece[i * step : (i + 1) * step]) for i in range(cuts)]
        down_far = [
            [jnp.concatenate([f[k][j] for f in fetched], 0) for j in range(n_sweep)]
            for k in range(len(others))
        ]

        g_all = [
            lax.all_gather(line_gather(x, "row", n_row), "dp", axis=0, tiled=True) for x in crossed
        ]
        g_own, g_far = g_all[0], g_all[1:]

        def share(far, j):
            at = lax.rem(s + j, n_sweep) * part
            return lax.dynamic_slice(far, (0, at), (far.shape[0], part))

        gate = dot(x_own, gate_own, PLAIN)
        up = dot(x_own, up_own, PLAIN)
        back = dot(g_own, down_own, COLS)
        for k in range(len(others)):
            for j in range(n_sweep):
                gate += dot(share(x_far[k], j), gate_far[k][j], PLAIN)
                up += dot(share(x_far[k], j), up_far[k][j], PLAIN)
                back += dot(share(g_far[k], j), down_far[k][j], COLS)
        sig = jax.nn.sigmoid(gate)
        silu = gate * sig
        hidden = (silu * up).astype(jnp.bfloat16)
        back = out_mult * back
        d_gate = (back * up * sig * (1.0 + gate * (1.0 - sig))).astype(jnp.bfloat16)
        d_up = (back * silu).astype(jnp.bfloat16)

        hidden_all = lax.all_gather(hidden, "dp", axis=0, tiled=False)
        mine = feats // n_dp
        g_mine = lax.dynamic_slice(g_own, (0, d * mine), (g_own.shape[0], mine))
        grad_down = out_mult * lax.dot_general(
            hidden_all, g_mine, (((1,), (0,)), ((), ())), preferred_element_type=jnp.float32
        )
        grad_down = grad_down.reshape(n_dp * width, mine)
        grad_gate = dot(x_own, d_gate, ROWS)
        grad_up = dot(x_own, d_up, ROWS)
        return grad_gate, grad_up, grad_down

    return local


def solution(mesh):
    return jax.shard_map(
        build(mesh),
        mesh=mesh,
        in_specs=(
            P(("sweep", "dp")),
            P("sweep"),
            P("row", "col"),
            P(("sweep", "dp", "row"), "col"),
            P("col", "row"),
            P("col", "row"),
            P("row", "col"),
        ),
        out_specs=(
            P(("sweep", "col"), ("row", "dp")),
            P(("sweep", "col"), ("row", "dp")),
            P(("sweep", "row"), ("col", "dp")),
        ),
        check_vma=False,
    )
```
